8 devices in a mesh: a3: 2 (over z, y), a2: 2 (over x), a1: 2 (over core).
Axes of the slice: x: 2, y: 2, z: 1, core: 2. Of those that a mesh axis runs over, the one named last changes fastest.
Arguments:
- tensor: bfloat16 [384, 720, 1440], P('a1', 'a2', 'a3')
- u_time: float32 [384, 48], replicated
- u_height: float32 [720, 88], replicated
- u_width: float32 [1440, 176], replicated
Outputs:
- output 1: float32 [384, 48], replicated
- output 2: float32 [720, 88], replicated
- output 3: float32 [1440, 176], replicated
- output 4: float32 [48, 88, 176], P('a1', 'a2', 'a3')
- output 5: float32 [], replicated
All inputs are finite; a program needn't handle non-finite values.
Results may differ from the reference program's by a relative error of at most 0.00743457.
Values are sent between devices in bfloat16 or wider.
A program may use at most 1 GiB of HBM per device.

```python
import jax
import jax.numpy as jnp
from jax import lax

FRAMES = 384
GRID_H = 720
GRID_W = 1440
RANK_T = 48
RANK_H = 88
RANK_W = 176
SIGNAL_RANK = 8


def setup_inputs(seed: int = 0) -> dict:
    key_list = jax.random.split(jax.random.key(seed), 8)
    fac_t = jax.random.normal(key_list[0], (FRAMES, SIGNAL_RANK), jnp.float32)
    fac_h = jax.random.normal(key_list[1], (GRID_H, SIGNAL_RANK), jnp.float32)
    fac_w = jax.random.normal(key_list[2], (GRID_W, SIGNAL_RANK), jnp.float32)
    weights = jax.random.uniform(key_list[3], (SIGNAL_RANK,), jnp.float32, 0.5, 1.5) * SIGNAL_RANK ** -0.5

    def one_frame(frame_idx):
        noise_map = jax.random.normal(jax.random.fold_in(key_list[4], frame_idx), (GRID_H, GRID_W), jnp.float32)
        signal = jnp.dot(fac_h * (fac_t[frame_idx] * weights), fac_w.T)
        return (signal + noise_map).astype(jnp.bfloat16)

    tensor = lax.map(one_frame, jnp.arange(FRAMES))
    u_time = jax.random.normal(key_list[5], (FRAMES, RANK_T), jnp.float32) * FRAMES ** -0.5
    u_height = jax.random.normal(key_list[6], (GRID_H, RANK_H), jnp.float32) * GRID_H ** -0.5
    u_width = jax.random.normal(key_list[7], (GRID_W, RANK_W), jnp.float32) * GRID_W ** -0.5
    return {'tensor': tensor, 'u_time': u_time, 'u_height': u_height, 'u_width': u_width}


def operand_f32(matrix):
    return matrix.astype(jnp.bfloat16).astype(jnp.float32)


def col_normalise(power_cols):
    return power_cols / jnp.sqrt(jnp.sum(power_cols * power_cols, axis=0, keepdims=True))


def gram_update(unfold, factor):
    gram_mat = jnp.dot(unfold, unfold.T, preferred_element_type=jnp.float32).astype(jnp.bfloat16)
    return col_normalise(jnp.dot(gram_mat, factor.astype(jnp.bfloat16), preferred_element_type=jnp.float32))


def reference(tensor, u_time, u_height, u_width):
    t_full = jnp.dot(tensor.reshape(FRAMES * GRID_H, GRID_W), u_width.astype(jnp.bfloat16), preferred_element_type=jnp.float32)
    t_mat = t_full.astype(jnp.bfloat16).reshape(FRAMES, GRID_H, RANK_W).astype(jnp.float32)
    y_one = jnp.einsum('ihc,hb->ibc', t_mat, operand_f32(u_height)).astype(jnp.bfloat16)
    new_time = gram_update(y_one.reshape(FRAMES, RANK_H * RANK_W), u_time)
    y_two = jnp.einsum('ihc,ia->hac', t_mat, operand_f32(new_time)).astype(jnp.bfloat16)
    new_height = gram_update(y_two.reshape(GRID_H, RANK_T * RANK_W), u_height)
    z_flat = jnp.dot(new_time.astype(jnp.bfloat16).T, tensor.reshape(FRAMES, GRID_H * GRID_W), preferred_element_type=jnp.float32)
    z_mat = z_flat.astype(jnp.bfloat16).reshape(RANK_T, GRID_H, GRID_W).astype(jnp.float32)
    y_three = jnp.einsum('ahw,hb->wab', z_mat, operand_f32(new_height)).astype(jnp.bfloat16)
    new_width = gram_update(y_three.reshape(GRID_W, RANK_T * RANK_H), u_width)
    core_tensor = jnp.einsum('wab,wc->abc', y_three.astype(jnp.float32), operand_f32(new_width))
    core_energy = jnp.sum(core_tensor * core_tensor)
    return new_time, new_height, new_width, core_tensor, core_energy
```

```python
import functools

import jax
import jax.numpy as jnp
from jax import lax
from jax.experimental import pallas as pl
from jax.experimental.pallas import tpu as pltpu
from jax.sharding import PartitionSpec as P

MESH = pl.DeviceIdType.MESH
F32, BF16 = jnp.float32, jnp.bfloat16
NT = (((1,), (1,)), ((), ()))

FR, GH, GW = 192, 360, 720
RT, RH, RW = 48, 88, 176
CH = 16
NCH = FR // CH
POS = CH * GH
NSUB = 3
SUB = POS // NSUB
CW = RW // 2
HP = 384
CL = 24


def coords():
    return lax.axis_index('a3'), lax.axis_index('a2'), lax.axis_index('a1')


def peer(me, k):
    flips = (k >> 2, (k >> 1) & 1, k & 1)
    return tuple(1 - m if f else m for m, f in zip(me, flips))


def flat(dev):
    return (dev[0] * 2 + dev[1]) * 2 + dev[2]


def remote(src, dst, send_sem, recv_sem, dev):
    return pltpu.make_async_remote_copy(src_ref=src, dst_ref=dst, send_sem=send_sem, recv_sem=recv_sem, device_id=dev, device_id_type=MESH)


def greet_all(me):
    barrier = pltpu.get_barrier_semaphore()
    for k in range(1, 8):
        pl.semaphore_signal(barrier, inc=1, device_id=peer(me, k), device_id_type=MESH)
    pl.semaphore_wait(barrier, 7)


def first_column(dev):
    return dev[1] * 40 + dev[2] * CL


def duplicate_rows(dev):
    return dev[1] * (1 - dev[2]) * (8 * CH)


def time_kernel(x_hbm, u3t_ref, u2p_ref, u1_ref, t_out, u1_out, xbuf, own, send, recv, sbuf, tbuf, t3, y1b, gram, gslots, pall,
                xsem, ysend, yrecv, credit, qsend, qrecv, gsend, grecv, psend, precv, osem):
    me = coords()
    y_peer = peer(me, 4)
    greet_all(me)

    def fetch(s, k):
        start = pl.multiple_of(s * POS + k * SUB, SUB)
        return pltpu.make_async_copy(x_hbm.at[pl.ds(start, SUB), :], xbuf.at[k], xsem.at[k])

    def lanes(k):
        return pl.ds(pl.multiple_of(k * SUB, 128), SUB)

    def ycopy(slot, k):
        return remote(send.at[slot, :, lanes(k)], recv.at[slot, :, lanes(k)], ysend.at[slot, k], yrecv.at[slot, k], y_peer)

    def qcopy(slot, q, t, src_dev):
        return remote(tbuf.at[slot, q - 1], t3.at[src_dev[2], t, src_dev[1]], qsend.at[slot, q - 1], qrecv.at[q - 1, t], peer(me, q))

    for k in range(NSUB):
        fetch(0, k).start()

    def produce(s):
        slot = lax.rem(s, 2)

        @pl.when(s >= 2)
        def _():
            pl.semaphore_wait(credit, 1)
            for k in range(NSUB):
                ycopy(slot, k).wait_send()

        def sub(k, carry):
            fetch(s, k).wait()
            part = lax.dot_general(u3t_ref[...], xbuf[k], NT, preferred_element_type=F32)
            own[slot, :, lanes(k)] = part[:CW]
            send[slot, :, lanes(k)] = part[CW:]
            ycopy(slot, k).start()

            @pl.when(s < NCH - 1)
            def _():
                fetch(s + 1, k).start()

            return carry

        lax.fori_loop(0, NSUB, sub, 0)

    def combine(t):
        slot = lax.rem(t, 2)
        for k in range(NSUB):
            ycopy(slot, k).wait_recv()
        lane = lax.broadcasted_iota(jnp.int32, (CW, 128), 1)
        for ii in range(CH):
            start = (ii * GH) // 128 * 128
            off = ii * GH - start
            wid = min(512, POS - start)
            blk = own[slot, :, start:start + wid] + recv[slot, :, start:start + wid]
            if off:
                blk = pltpu.roll(blk, wid - off, 1)
            for lt in range(3):
                piece = blk[:, lt * 128:(lt + 1) * 128]
                sbuf[lt, pl.ds(ii, CW, stride=CH), :] = piece if lt < 2 else jnp.where(lane < GH - 256, piece, 0.0)

        @pl.when(t < NCH - 2)
        def _():
            pl.semaphore_signal(credit, inc=1, device_id=y_peer, device_id_type=MESH)

        @pl.when(t >= 2)
        def _():
            for q in range(1, 4):
                qcopy(slot, q, t - 2, me).wait_send()

        row = lax.broadcasted_iota(jnp.int32, (CL * CH, 128), 0)

        def part_for(dev, put):
            for lt in range(3):
                v = sbuf[lt, pl.ds(pl.multiple_of(first_column(dev) * CH, 8), CL * CH), :]
                put(slice(lt * 128, (lt + 1) * 128), jnp.where(row < duplicate_rows(dev), 0.0, v).astype(BF16))

        for q in range(1, 4):
            def put_peer(ls, v):
                tbuf[slot, q - 1, :, ls] = v

            part_for(peer(me, q), put_peer)
            qcopy(slot, q, t, me).start()

        def put_own(ls, v):
            t3[me[2], t, me[1], :, ls] = v

        part_for(me, put_own)

    def height(t):
        for q in range(1, 4):
            qcopy(0, q, t, peer(me, q)).wait_recv()
        for aa in range(2):
            acc = jnp.dot(t3[aa, t, 0], u2p_ref[0], preferred_element_type=F32)
            acc = acc + jnp.dot(t3[aa, t, 1], u2p_ref[1], preferred_element_type=F32)
            acc = acc.astype(BF16).reshape(CL // 2, 2, CH, 128)
            rows = pl.ds(pl.multiple_of(aa * FR + t * CH, CH), CH)
            y1b[:, rows, 0:128] = acc[:, 0]
            y1b[:, rows, 128:256] = acc[:, 1]

    def step(s, carry):
        @pl.when(s < NCH)
        def _():
            produce(s)

        @pl.when((s >= 1) & (s <= NCH))
        def _():
            combine(s - 1)

        @pl.when(s >= 2)
        def _():
            height(s - 2)

        return carry

    lax.fori_loop(0, NCH + 2, step, 0)

    for slot in range(2):
        for k in range(NSUB):
            ycopy(slot, k).wait_send()
        for q in range(1, 4):
            qcopy(slot, q, NCH - 2 + slot, me).wait_send()

    keep = pltpu.make_async_copy(t3, t_out, osem)
    keep.start()

    acc = lax.dot_general(y1b[0], y1b[0], NT, preferred_element_type=F32)
    for c in range(1, CL // 2):
        acc = acc + lax.dot_general(y1b[c], y1b[c], NT, preferred_element_type=F32)
    gram[...] = acc

    def rows_of(dev):
        return pl.ds(pl.multiple_of(flat(dev) * RT, 8), RT)

    def gcopy(k):
        return remote(gram.at[rows_of(peer(me, k))], gslots.at[k - 1], gsend.at[k - 1], grecv.at[k - 1], peer(me, k))

    for k in range(1, 8):
        gcopy(k).start()
    total = gram[rows_of(me), :]
    for k in range(1, 8):
        gcopy(k).wait_recv()
        total = total + gslots[k - 1]
    pall[flat(me)] = jnp.dot(total.astype(BF16), u1_ref[...], preferred_element_type=F32)

    def pcopy(k, dev):
        return remote(pall.at[flat(me)], pall.at[flat(dev)], psend.at[k - 1], precv.at[k - 1], peer(me, k))

    for k in range(1, 8):
        pcopy(k, me).start()
    for k in range(1, 8):
        pcopy(k, peer(me, k)).wait_recv()
    power = pall[...].reshape(8 * RT, 128)[:, :RT]
    u1_out[...] = power / jnp.sqrt(jnp.sum(power * power, axis=0, keepdims=True))
    for k in range(1, 8):
        gcopy(k).wait_send()
        pcopy(k, me).wait_send()
    keep.wait()


def time_phase(x2d, u3t, u2p, u1p):
    vmem, anym = pl.BlockSpec(memory_space=pltpu.VMEM), pl.BlockSpec(memory_space=pl.ANY)
    dma = pltpu.SemaphoreType.DMA
    return pl.pallas_call(
        time_kernel,
        name='time_phase',
        out_shape=(jax.ShapeDtypeStruct((2, NCH, 2, CL * CH, HP), BF16), jax.ShapeDtypeStruct((2 * FR, RT), F32)),
        in_specs=[anym, vmem, vmem, vmem],
        out_specs=(anym, vmem),
        scratch_shapes=[
            pltpu.VMEM((NSUB, SUB, GW), BF16), pltpu.VMEM((2, CW, POS), F32), pltpu.VMEM((2, CW, POS), F32), pltpu.VMEM((2, CW, POS), F32),
            pltpu.VMEM((3, CW * CH, 128), F32), pltpu.VMEM((2, 3, CL * CH, HP), BF16), pltpu.VMEM((2, NCH, 2, CL * CH, HP), BF16),
            pltpu.VMEM((CL // 2, 2 * FR, 256), BF16), pltpu.VMEM((2 * FR, 2 * FR), F32), pltpu.VMEM((7, RT, 2 * FR), F32), pltpu.VMEM((8, RT, 128), F32),
            dma((NSUB,)), dma((2, NSUB)), dma((2, NSUB)), pltpu.SemaphoreType.REGULAR, dma((2, 3)), dma((3, NCH)),
            dma((7,)), dma((7,)), dma((7,)), dma((7,)), dma(()),
        ],
        compiler_params=pltpu.CompilerParams(collective_id=0, has_side_effects=True, vmem_limit_bytes=60 << 20),
    )(x2d, u3t, u2p, u1p)


def rows_of(factor, axis_name, count):
    start_row = lax.axis_index(axis_name) * count
    return lax.dynamic_slice_in_dim(factor, start_row, count, 0).astype(BF16)


def gram_update(local_rows, row_axes, sum_axes, factor):
    all_rows = lax.all_gather(local_rows, row_axes, axis=0, tiled=True)
    gram_part = lax.dot_general(local_rows, all_rows, NT, preferred_element_type=F32)
    gram_rows = lax.psum(gram_part, sum_axes).astype(BF16)
    power_cols = jnp.dot(gram_rows, factor.astype(BF16), preferred_element_type=F32)
    col_sq = lax.psum(jnp.sum(power_cols * power_cols, axis=0, keepdims=True), row_axes)
    return lax.all_gather(power_cols / jnp.sqrt(col_sq), row_axes, axis=0, tiled=True)


def solution(mesh):
    def local_sweep(tensor, u_time, u_height, u_width):
        frames, grid_h, grid_w = tensor.shape
        y = lax.axis_index('a3')
        u3 = rows_of(u_width, 'a3', grid_w).T
        u3t = jnp.concatenate([lax.dynamic_slice_in_dim(u3, y * CW, CW, 0), lax.dynamic_slice_in_dim(u3, (1 - y) * CW, CW, 0)], 0)
        u2p = jnp.pad(u_height.astype(BF16).reshape(2, grid_h, RH), ((0, 0), (0, HP - grid_h), (0, 128 - RH)))
        u1p = jnp.pad(u_time.astype(BF16), ((0, 0), (0, 128 - RT)))
        t3, new_time = time_phase(tensor.reshape(frames * grid_h, grid_w), u3t, u2p, u1p)
        t3 = t3.reshape(2, NCH, 2, CL, CH, HP)
        y_two = jnp.einsum('Asxcih,Asir->xcrh', t3, new_time.astype(BF16).reshape(2, NCH, CH, RT), preferred_element_type=F32).astype(BF16)
        gram_part = jnp.einsum('xcrh,zcrk->xhzk', y_two, y_two, preferred_element_type=F32)[:, :grid_h, :, :grid_h].reshape(2 * grid_h, 2 * grid_h)
        gram_two = lax.psum(gram_part, ('a1', 'a2', 'a3')).astype(BF16)
        power = jnp.dot(gram_two, u_height.astype(BF16), preferred_element_type=F32)
        new_height = power / jnp.sqrt(jnp.sum(power * power, axis=0, keepdims=True))

        time_rows = rows_of(new_time, 'a1', frames)
        z_part = lax.dot_general(time_rows, tensor, (((0,), (0,)), ((), ())), preferred_element_type=F32)
        z_mat = lax.psum_scatter(z_part, 'a1', scatter_dimension=0, tiled=True).astype(BF16)
        y3_part = jnp.einsum('ahw,hb->wab', z_mat, rows_of(new_height, 'a2', grid_h), preferred_element_type=F32)
        y_three = lax.psum_scatter(y3_part, 'a2', scatter_dimension=2, tiled=True).astype(BF16)
        new_width = gram_update(y_three.reshape(grid_w, -1), 'a3', ('a1', 'a2'), u_width)
        core_part = jnp.einsum('wab,wc->abc', y_three, rows_of(new_width, 'a3', grid_w), preferred_element_type=F32)
        core_tensor = lax.psum_scatter(core_part, 'a3', scatter_dimension=2, tiled=True)
        core_energy = lax.psum(jnp.sum(core_tensor * core_tensor), ('a1', 'a2', 'a3'))
        return new_time, new_height, new_width, core_tensor, core_energy

    return jax.shard_map(local_sweep, mesh=mesh, in_specs=(P('a1', 'a2', 'a3'), P(), P(), P()), out_specs=(P(), P(), P(), P('a1', 'a2', 'a3'), P()), check_vma=False)
```

```python
import functools

import jax
import jax.numpy as jnp
from jax import lax
from jax.experimental import pallas as pl
from jax.experimental.pallas import tpu as pltpu
from jax.sharding import PartitionSpec as P

MESH = pl.DeviceIdType.MESH
F32, BF16 = jnp.float32, jnp.bfloat16
NT = (((1,), (1,)), ((), ()))

FR, GH, GW = 192, 360, 720
RT, RH, RW = 48, 88, 176
CH = 16
NCH = FR // CH
POS = CH * GH
NSUB = 3
SUB = POS // NSUB
CW = RW // 2
HP = 384
CL = 24


def coords():
    return lax.axis_index('a3'), lax.axis_index('a2'), lax.axis_index('a1')


def peer(me, k):
    flips = (k >> 2, (k >> 1) & 1, k & 1)
    return tuple(1 - m if f else m for m, f in zip(me, flips))


def flat(dev):
    return (dev[0] * 2 + dev[1]) * 2 + dev[2]


def remote(src, dst, send_sem, recv_sem, dev):
    return pltpu.make_async_remote_copy(src_ref=src, dst_ref=dst, send_sem=send_sem, recv_sem=recv_sem, device_id=dev, device_id_type=MESH)


def greet_all(me):
    barrier = pltpu.get_barrier_semaphore()
    for k in range(1, 8):
        pl.semaphore_signal(barrier, inc=1, device_id=peer(me, k), device_id_type=MESH)
    pl.semaphore_wait(barrier, 7)


def first_column(dev):
    return dev[1] * 40 + dev[2] * CL


def duplicate_rows(dev):
    return dev[1] * (1 - dev[2]) * (8 * CH)


def time_kernel(x_hbm, u3t_ref, u2p_ref, u1_ref, t_out, u1_out, xbuf, own, send, recv, sbuf, tbuf, t3, y1b, gram, gslots, pall,
                xsem, ysend, yrecv, credit, qsend, qrecv, gsend, grecv, psend, precv, osem):
    me = coords()
    y_peer = peer(me, 4)
    greet_all(me)

    def fetch(s, k):
        start = pl.multiple_of(s * POS + k * SUB, SUB)
        return pltpu.make_async_copy(x_hbm.at[pl.ds(start, SUB), :], xbuf.at[k], xsem.at[k])

    def lanes(k):
        return pl.ds(pl.multiple_of(k * SUB, 128), SUB)

    def ycopy(slot, k):
        return remote(send.at[slot, :, lanes(k)], recv.at[slot, :, lanes(k)], ysend.at[slot, k], yrecv.at[slot, k], y_peer)

    def qcopy(slot, q, t, src_dev):
        return remote(tbuf.at[slot, q - 1], t3.at[src_dev[2], t, src_dev[1]], qsend.at[slot, q - 1], qrecv.at[q - 1, t], peer(me, q))

    for k in range(NSUB):
        fetch(0, k).start()

    def produce(s):
        slot = lax.rem(s, 2)

        @pl.when(s >= 2)
        def _():
            pl.semaphore_wait(credit, 1)
            for k in range(NSUB):
                ycopy(slot, k).wait_send()

        def sub(k, carry):
            fetch(s, k).wait()
            part = lax.dot_general(u3t_ref[...], xbuf[k], NT, preferred_element_type=F32)
            own[slot, :, lanes(k)] = part[:CW]
            send[slot, :, lanes(k)] = part[CW:]
            ycopy(slot, k).start()

            @pl.when(s < NCH - 1)
            def _():
                fetch(s + 1, k).start()

            return carry

        lax.fori_loop(0, NSUB, sub, 0)

    def combine(t):
        slot = lax.rem(t, 2)
        for k in range(NSUB):
            ycopy(slot, k).wait_recv()
        lane = lax.broadcasted_iota(jnp.int32, (CW, 128), 1)
        for ii in range(CH):
            start = (ii * GH) // 128 * 128
            off = ii * GH - start
            wid = min(512, POS - start)
            blk = own[slot, :, start:start + wid] + recv[slot, :, start:start + wid]
            if off:
                blk = pltpu.roll(blk, wid - off, 1)
            for lt in range(3):
                piece = blk[:, lt * 128:(lt + 1) * 128]
                sbuf[lt, pl.ds(ii, CW, stride=CH), :] = piece if lt < 2 else jnp.where(lane < GH - 256, piece, 0.0)

        @pl.when(t < NCH - 2)
        def _():
            pl.semaphore_signal(credit, inc=1, device_id=y_peer, device_id_type=MESH)

        @pl.when(t >= 2)
        def _():
            for q in range(1, 4):
                qcopy(slot, q, t - 2, me).wait_send()

        row = lax.broadcasted_iota(jnp.int32, (CL * CH, 128), 0)

        def part_for(dev, put):
            for lt in range(3):
                v = sbuf[lt, pl.ds(pl.multiple_of(first_column(dev) * CH, 8), CL * CH), :]
                put(slice(lt * 128, (lt + 1) * 128), jnp.where(row < duplicate_rows(dev), 0.0, v).astype(BF16))

        for q in range(1, 4):
            def put_peer(ls, v):
                tbuf[slot, q - 1, :, ls] = v

            part_for(peer(me, q), put_peer)
            qcopy(slot, q, t, me).start()

        def put_own(ls, v):
            t3[me[2], t, me[1], :, ls] = v

        part_for(me, put_own)

    def height(t):
        for q in range(1, 4):
            qcopy(0, q, t, peer(me, q)).wait_recv()
        for aa in range(2):
            acc = jnp.dot(t3[aa, t, 0], u2p_ref[0], preferred_element_type=F32)
            acc = acc + jnp.dot(t3[aa, t, 1], u2p_ref[1], preferred_element_type=F32)
            acc = acc.astype(BF16).reshape(CL // 2, 2, CH, 128)
            rows = pl.ds(pl.multiple_of(aa * FR + t * CH, CH), CH)
            y1b[:, rows, 0:128] = acc[:, 0]
            y1b[:, rows, 128:256] = acc[:, 1]

    def step(s, carry):
        @pl.when(s < NCH)
        def _():
            produce(s)

        @pl.when((s >= 1) & (s <= NCH))
        def _():
            combine(s - 1)

        @pl.when(s >= 2)
        def _():
            height(s - 2)

        return carry

    lax.fori_loop(0, NCH + 2, step, 0)

    for slot in range(2):
        for k in range(NSUB):
            ycopy(slot, k).wait_send()
        for q in range(1, 4):
            qcopy(slot, q, NCH - 2 + slot, me).wait_send()

    keep = pltpu.make_async_copy(t3, t_out, osem)
    keep.start()

    acc = lax.dot_general(y1b[0], y1b[0], NT, preferred_element_type=F32)
    for c in range(1, CL // 2):
        acc = acc + lax.dot_general(y1b[c], y1b[c], NT, preferred_element_type=F32)
    gram[...] = acc

    def rows_of(dev):
        return pl.ds(pl.multiple_of(flat(dev) * RT, 8), RT)

    def gcopy(k):
        return remote(gram.at[rows_of(peer(me, k))], gslots.at[k - 1], gsend.at[k - 1], grecv.at[k - 1], peer(me, k))

    for k in range(1, 8):
        gcopy(k).start()
    total = gram[rows_of(me), :]
    for k in range(1, 8):
        gcopy(k).wait_recv()
        total = total + gslots[k - 1]
    pall[flat(me)] = jnp.dot(total.astype(BF16), u1_ref[...], preferred_element_type=F32)

    def pcopy(k, dev):
        return remote(pall.at[flat(me)], pall.at[flat(dev)], psend.at[k - 1], precv.at[k - 1], peer(me, k))

    for k in range(1, 8):
        pcopy(k, me).start()
    for k in range(1, 8):
        pcopy(k, peer(me, k)).wait_recv()
    power = pall[...].reshape(8 * RT, 128)[:, :RT]
    u1_out[...] = power / jnp.sqrt(jnp.sum(power * power, axis=0, keepdims=True))
    for k in range(1, 8):
        gcopy(k).wait_send()
        pcopy(k, me).wait_send()
    keep.wait()


def time_phase(x2d, u3t, u2p, u1p):
    vmem, anym = pl.BlockSpec(memory_space=pltpu.VMEM), pl.BlockSpec(memory_space=pl.ANY)
    dma = pltpu.SemaphoreType.DMA
    return pl.pallas_call(
        time_kernel,
        name='time_phase',
        out_shape=(jax.ShapeDtypeStruct((2, NCH, 2, CL * CH, HP), BF16), jax.ShapeDtypeStruct((2 * FR, RT), F32)),
        in_specs=[anym, vmem, vmem, vmem],
        out_specs=(anym, vmem),
        scratch_shapes=[
            pltpu.VMEM((NSUB, SUB, GW), BF16), pltpu.VMEM((2, CW, POS), F32), pltpu.VMEM((2, CW, POS), F32), pltpu.VMEM((2, CW, POS), F32),
            pltpu.VMEM((3, CW * CH, 128), F32), pltpu.VMEM((2, 3, CL * CH, HP), BF16), pltpu.VMEM((2, NCH, 2, CL * CH, HP), BF16),
            pltpu.VMEM((CL // 2, 2 * FR, 256), BF16), pltpu.VMEM((2 * FR, 2 * FR), F32), pltpu.VMEM((7, RT, 2 * FR), F32), pltpu.VMEM((8, RT, 128), F32),
            dma((NSUB,)), dma((2, NSUB)), dma((2, NSUB)), pltpu.SemaphoreType.REGULAR, dma((2, 3)), dma((3, NCH)),
            dma((7,)), dma((7,)), dma((7,)), dma((7,)), dma(()),
        ],
        compiler_params=pltpu.CompilerParams(collective_id=0, has_side_effects=True, vmem_limit_bytes=60 << 20),
    )(x2d, u3t, u2p, u1p)


NPAIR = 12
PR = RH
WP = 768
WQ = WP // 4


def width_kernel(z_hbm, u2t_ref, u3p_ref, u3_out, g_out, e_out, zbuf, own, send, recv, y3, acc, core_in, x_in, pall, u3b, energy,
                 zsem, xsend, xrecv, ysend, yrecv, csend, crecv, rsend, rrecv, psend, precv, fsend, frecv, esend, erecv):
    me = coords()
    y, x, a = me
    x_peer, y_peer, c_peer = peer(me, 2), peer(me, 4), peer(me, 1)
    greet_all(me)

    def fetch(p, slot):
        return pltpu.make_async_copy(z_hbm.at[pl.ds(p * 2, 2)], zbuf.at[slot], zsem.at[slot])

    def xcopy(p):
        return remote(send.at[p], recv.at[p], xsend.at[p], xrecv.at[p], x_peer)

    def ycopy(p):
        return remote(y3.at[0, p], y3.at[1, p], ysend.at[p], yrecv.at[p], y_peer)

    fetch(0, 0).start()
    acc[...] = jnp.zeros_like(acc)

    def produce(p, carry):
        slot = lax.rem(p, 2)
        fetch(p, slot).wait()

        @pl.when(p < NPAIR - 1)
        def _():
            fetch(p + 1, 1 - slot).start()

        for r in range(2):
            part = jnp.dot(u2t_ref[...], zbuf[slot, r], preferred_element_type=F32)
            own[p, r * 44:(r + 1) * 44] = part[0:44]
            send[p, r * 44:(r + 1) * 44] = part[48:92]
        xcopy(p).start()
        return carry

    lax.fori_loop(0, NPAIR, produce, 0)

    def add_gram(p):
        ycopy(p).wait_recv()

        def block(m, carry):
            cols = pl.ds(pl.multiple_of(m * 128, 128), 128)
            lhs = y3[0, p, :, cols]
            for half in range(2):
                add = lax.dot_general(lhs, y3[half, p], (((0,), (0,)), ((), ())), preferred_element_type=F32)
                acc[cols, half * WP:(half + 1) * WP] += add
            return carry

        lax.fori_loop(0, WP // 128, block, 0)

    def consume(p, carry):
        @pl.when(p < NPAIR)
        def _():
            xcopy(p).wait_recv()
            y3[0, p, :, 640:768] = jnp.zeros((PR, 128), BF16)
            y3[0, p, :, 0:GW] = (own[p] + recv[p]).astype(BF16)
            ycopy(p).start()

        @pl.when(p >= 1)
        def _():
            add_gram(p - 1)

        return carry

    lax.fori_loop(0, NPAIR + 1, consume, 0)

    def quarter(core, side):
        return pl.ds(pl.multiple_of(core * 2 * WQ + side * WQ, 8), WQ)

    def ccopy(i):
        side = 1 - x if i == 0 else x
        return remote(acc.at[quarter(1 - a, side)], core_in.at[i], csend.at[i], crecv.at[i], c_peer)

    ccopy(0).start()
    ccopy(1).start()
    ccopy(0).wait_recv()
    acc[quarter(a, 1 - x), :] += core_in[0]
    rcopy = remote(acc.at[quarter(a, 1 - x)], x_in, rsend, rrecv, x_peer)
    rcopy.start()
    ccopy(1).wait_recv()
    rows = acc[quarter(a, x), :] + core_in[1]
    rcopy.wait_recv()
    rows = (rows + x_in[...]).astype(BF16)

    def slot_of(dev):
        return dev[0] * 4 + dev[2] * 2 + dev[1]

    mine = slot_of(me)
    pall[mine] = jnp.dot(rows, u3p_ref[...], preferred_element_type=F32)

    def pcopy(i, dev):
        return remote(pall.at[slot_of(dev)], pall.at[slot_of(dev)], psend.at[i], precv.at[i], peer(me, (2, 4, 6)[i]))

    def fcopy(i, dev):
        return remote(pall.at[slot_of(dev)], pall.at[slot_of(dev)], fsend.at[i], frecv.at[i], c_peer)

    for i in range(3):
        pcopy(i, me).start()
    fcopy(3, me).start()
    for i in range(3):
        dev = peer(me, (2, 4, 6)[i])
        pcopy(i, dev).wait_recv()
        fcopy(i, dev).start()
    for i in range(3):
        fcopy(i, peer(c_peer, (2, 4, 6)[i])).wait_recv()
    fcopy(3, c_peer).wait_recv()
    power = pall[...].reshape(2 * WP, 256)
    lane = lax.broadcasted_iota(jnp.int32, (1, 256), 1)
    norm = jnp.where(lane < RW, jnp.sqrt(jnp.sum(power * power, axis=0, keepdims=True)), 1.0)
    fresh = power / norm
    u3_out[0:GW, :] = fresh[0:GW, :RW]
    u3_out[GW:2 * GW, :] = fresh[WP:WP + GW, :RW]
    half = pltpu.roll(fresh, 256 - y * CW, 1)[:, :128].astype(BF16)
    u3b[...] = half.reshape(2, WP, 128)

    def core_rows(p, esum):
        g = jnp.dot(y3[0, p], u3b[y], preferred_element_type=F32) + jnp.dot(y3[1, p], u3b[1 - y], preferred_element_type=F32)
        g = jnp.where(lane[:, :128] < CW, g, 0.0)
        g_out[p] = g[:, :CW]
        return esum + jnp.sum((g * g).reshape(PR // 8, 8, 128), axis=0)

    energy[flat(me)] = lax.fori_loop(0, NPAIR, core_rows, jnp.zeros((8, 128), F32))

    def ecopy(k, dev):
        return remote(energy.at[flat(dev)], energy.at[flat(dev)], esend.at[k - 1], erecv.at[k - 1], peer(me, k))

    for k in range(1, 8):
        ecopy(k, me).start()
    for k in range(1, 8):
        ecopy(k, peer(me, k)).wait_recv()
    e_out[...] = jnp.sum(jnp.sum(energy[...], axis=0), axis=(0, 1), keepdims=True)

    def drain(p, carry):
        xcopy(p).wait_send()
        ycopy(p).wait_send()
        return carry

    lax.fori_loop(0, NPAIR, drain, 0)
    ccopy(0).wait_send()
    ccopy(1).wait_send()
    rcopy.wait_send()
    for i in range(3):
        pcopy(i, me).wait_send()
    for i in range(4):
        fcopy(i, me).wait_send()
    for k in range(1, 8):
        ecopy(k, me).wait_send()


def width_phase(z_mat, u2t, u3p):
    vmem, anym = pl.BlockSpec(memory_space=pltpu.VMEM), pl.BlockSpec(memory_space=pl.ANY)
    dma = pltpu.SemaphoreType.DMA
    return pl.pallas_call(
        width_kernel,
        name='width_phase',
        out_shape=(jax.ShapeDtypeStruct((2 * GW, RW), F32), jax.ShapeDtypeStruct((NPAIR, PR, CW), F32), jax.ShapeDtypeStruct((1, 1), F32)),
        in_specs=[anym, vmem, vmem],
        out_specs=(vmem, vmem, vmem),
        scratch_shapes=[
            pltpu.VMEM((2, 2, GH, GW), BF16), pltpu.VMEM((NPAIR, PR, GW), F32), pltpu.VMEM((NPAIR, PR, GW), F32), pltpu.VMEM((NPAIR, PR, GW), F32),
            pltpu.VMEM((2, NPAIR, PR, WP), BF16), pltpu.VMEM((WP, 2 * WP), F32), pltpu.VMEM((2, WQ, 2 * WP), F32), pltpu.VMEM((WQ, 2 * WP), F32),
            pltpu.VMEM((8, WQ, 256), F32), pltpu.VMEM((2, WP, 128), BF16), pltpu.VMEM((8, 8, 128), F32),
            dma((2,)), dma((NPAIR,)), dma((NPAIR,)), dma((NPAIR,)), dma((NPAIR,)), dma((2,)), dma((2,)), dma(()), dma(()),
            dma((3,)), dma((3,)), dma((4,)), dma((4,)), dma((7,)), dma((7,)),
        ],
        compiler_params=pltpu.CompilerParams(collective_id=1, has_side_effects=True, vmem_limit_bytes=60 << 20),
    )(z_mat, u2t, u3p)


def rows_of(factor, axis_name, count):
    start_row = lax.axis_index(axis_name) * count
    return lax.dynamic_slice_in_dim(factor, start_row, count, 0).astype(BF16)


def solution(mesh):
    def local_sweep(tensor, u_time, u_height, u_width):
        frames, grid_h, grid_w = tensor.shape
        y = lax.axis_index('a3')
        u3 = rows_of(u_width, 'a3', grid_w).T
        u3t = jnp.concatenate([lax.dynamic_slice_in_dim(u3, y * CW, CW, 0), lax.dynamic_slice_in_dim(u3, (1 - y) * CW, CW, 0)], 0)
        u2p = jnp.pad(u_height.astype(BF16).reshape(2, grid_h, RH), ((0, 0), (0, HP - grid_h), (0, 128 - RH)))
        u1p = jnp.pad(u_time.astype(BF16), ((0, 0), (0, 128 - RT)))
        t3, new_time = time_phase(tensor.reshape(frames * grid_h, grid_w), u3t, u2p, u1p)
        t3 = t3.reshape(2, NCH, 2, CL, CH, HP)
        y_two = jnp.einsum('Asxcih,Asir->xcrh', t3, new_time.astype(BF16).reshape(2, NCH, CH, RT), preferred_element_type=F32).astype(BF16)
        gram_part = jnp.einsum('xcrh,zcrk->xhzk', y_two, y_two, preferred_element_type=F32)[:, :grid_h, :, :grid_h].reshape(2 * grid_h, 2 * grid_h)
        gram_two = lax.psum(gram_part, ('a1', 'a2', 'a3')).astype(BF16)
        power = jnp.dot(gram_two, u_height.astype(BF16), preferred_element_type=F32)
        new_height = power / jnp.sqrt(jnp.sum(power * power, axis=0, keepdims=True))

        time_rows = rows_of(new_time, 'a1', frames)
        z_part = lax.dot_general(time_rows, tensor, (((0,), (0,)), ((), ())), preferred_element_type=F32)
        z_mat = lax.psum_scatter(z_part, 'a1', scatter_dimension=0, tiled=True).astype(BF16)
        x = lax.axis_index('a2')
        u2r = rows_of(new_height, 'a2', grid_h).T
        own_b, other_b = lax.dynamic_slice_in_dim(u2r, x * 44, 44, 0), lax.dynamic_slice_in_dim(u2r, (1 - x) * 44, 44, 0)
        u2t = jnp.concatenate([jnp.pad(own_b, ((0, 4), (0, 0))), jnp.pad(other_b, ((0, 4), (0, 0)))], 0)
        u3y = jnp.pad(u_width.astype(BF16).reshape(2, grid_w, RW), ((0, 0), (0, WP - grid_w), (0, 256 - RW)))
        u3p = jnp.concatenate([lax.dynamic_slice_in_dim(u3y, y, 1, 0), lax.dynamic_slice_in_dim(u3y, 1 - y, 1, 0)], 0).reshape(2 * WP, 256)
        new_width, core_tensor, core_energy = width_phase(z_mat, u2t, u3p)
        core_tensor = core_tensor.reshape(RT // 2, RH // 2, CW)
        core_energy = core_energy.reshape(())
        return new_time, new_height, new_width, core_tensor, core_energy

    return jax.shard_map(local_sweep, mesh=mesh, in_specs=(P('a1', 'a2', 'a3'), P(), P(), P()), out_specs=(P(), P(), P(), P('a1', 'a2', 'a3'), P()), check_vma=False)
```

```python
import functools

import jax
import jax.numpy as jnp
from jax import lax
from jax.experimental import pallas as pl
from jax.experimental.pallas import tpu as pltpu
from jax.sharding import PartitionSpec as P

MESH = pl.DeviceIdType.MESH
F32, BF16 = jnp.float32, jnp.bfloat16
NT = (((1,), (1,)), ((), ()))

FR, GH, GW = 192, 360, 720
RT, RH, RW = 48, 88, 176
CH = 16
NCH = FR // CH
POS = CH * GH
NSUB = 3
SUB = POS // NSUB
CW = RW // 2
HP = 384
CL = 24


def coords():
    return lax.axis_index('a3'), lax.axis_index('a2'), lax.axis_index('a1')


def peer(me, k):
    flips = (k >> 2, (k >> 1) & 1, k & 1)
    return tuple(1 - m if f else m for m, f in zip(me, flips))


def flat(dev):
    return (dev[0] * 2 + dev[1]) * 2 + dev[2]


def remote(src, dst, send_sem, recv_sem, dev):
    return pltpu.make_async_remote_copy(src_ref=src, dst_ref=dst, send_sem=send_sem, recv_sem=recv_sem, device_id=dev, device_id_type=MESH)


def greet_all(me):
    barrier = pltpu.get_barrier_semaphore()
    for k in range(1, 8):
        pl.semaphore_signal(barrier, inc=1, device_id=peer(me, k), device_id_type=MESH)
    pl.semaphore_wait(barrier, 7)


def first_column(dev):
    return dev[1] * 40 + dev[2] * CL


def duplicate_rows(dev):
    return dev[1] * (1 - dev[2]) * (8 * CH)


def time_kernel(x_hbm, u3t_ref, u2p_ref, u1_ref, t_out, u1_out, xbuf, own, send, recv, sbuf, tbuf, t3, y1b, gram, gslots, pall,
                xsem, ysend, yrecv, credit, qsend, qrecv, gsend, grecv, psend, precv, osem):
    me = coords()
    y_peer = peer(me, 4)
    greet_all(me)

    def fetch(s, k):
        start = pl.multiple_of(s * POS + k * SUB, SUB)
        return pltpu.make_async_copy(x_hbm.at[pl.ds(start, SUB), :], xbuf.at[k], xsem.at[k])

    def lanes(k):
        return pl.ds(pl.multiple_of(k * SUB, 128), SUB)

    def ycopy(slot, k):
        return remote(send.at[slot, :, lanes(k)], recv.at[slot, :, lanes(k)], ysend.at[slot, k], yrecv.at[slot, k], y_peer)

    def qcopy(slot, q, t, src_dev):
        return remote(tbuf.at[slot, q - 1], t3.at[src_dev[2], t, src_dev[1]], qsend.at[slot, q - 1], qrecv.at[q - 1, t], peer(me, q))

    for k in range(NSUB):
        fetch(0, k).start()

    def produce(s):
        slot = lax.rem(s, 2)

        @pl.when(s >= 2)
        def _():
            pl.semaphore_wait(credit, 1)
            for k in range(NSUB):
                ycopy(slot, k).wait_send()

        def sub(k, carry):
            fetch(s, k).wait()
            part = lax.dot_general(u3t_ref[...], xbuf[k], NT, preferred_element_type=F32)
            own[slot, :, lanes(k)] = part[:CW]
            send[slot, :, lanes(k)] = part[CW:]
            ycopy(slot, k).start()

            @pl.when(s < NCH - 1)
            def _():
                fetch(s + 1, k).start()

            return carry

        lax.fori_loop(0, NSUB, sub, 0)

    def combine(t):
        slot = lax.rem(t, 2)
        for k in range(NSUB):
            ycopy(slot, k).wait_recv()
        lane = lax.broadcasted_iota(jnp.int32, (CW, 128), 1)
        for ii in range(CH):
            start = (ii * GH) // 128 * 128
            off = ii * GH - start
            wid = min(512, POS - start)
            blk = own[slot, :, start:start + wid] + recv[slot, :, start:start + wid]
            if off:
                blk = pltpu.roll(blk, wid - off, 1)
            for lt in range(3):
                piece = blk[:, lt * 128:(lt + 1) * 128]
                sbuf[lt, pl.ds(ii, CW, stride=CH), :] = piece if lt < 2 else jnp.where(lane < GH - 256, piece, 0.0)

        @pl.when(t < NCH - 2)
        def _():
            pl.semaphore_signal(credit, inc=1, device_id=y_peer, device_id_type=MESH)

        @pl.when(t >= 2)
        def _():
            for q in range(1, 4):
                qcopy(slot, q, t - 2, me).wait_send()

        row = lax.broadcasted_iota(jnp.int32, (CL * CH, 128), 0)

        def part_for(dev, put):
            for lt in range(3):
                v = sbuf[lt, pl.ds(pl.multiple_of(first_column(dev) * CH, 8), CL * CH), :]
                put(slice(lt * 128, (lt + 1) * 128), jnp.where(row < duplicate_rows(dev), 0.0, v).astype(BF16))

        for q in range(1, 4):
            def put_peer(ls, v):
                tbuf[slot, q - 1, :, ls] = v

            part_for(peer(me, q), put_peer)
            qcopy(slot, q, t, me).start()

        def put_own(ls, v):
            t3[me[2], t, me[1], :, ls] = v

        part_for(me, put_own)

    def height(t):
        for q in range(1, 4):
            qcopy(0, q, t, peer(me, q)).wait_recv()
        for aa in range(2):
            acc = jnp.dot(t3[aa, t, 0], u2p_ref[0], preferred_element_type=F32)
            acc = acc + jnp.dot(t3[aa, t, 1], u2p_ref[1], preferred_element_type=F32)
            acc = acc.astype(BF16).reshape(CL // 2, 2, CH, 128)
            rows = pl.ds(pl.multiple_of(aa * FR + t * CH, CH), CH)
            y1b[:, rows, 0:128] = acc[:, 0]
            y1b[:, rows, 128:256] = acc[:, 1]

    def step(s, carry):
        @pl.when(s < NCH)
        def _():
            produce(s)

        @pl.when((s >= 1) & (s <= NCH))
        def _():
            combine(s - 1)

        @pl.when(s >= 2)
        def _():
            height(s - 2)

        return carry

    lax.fori_loop(0, NCH + 2, step, 0)

    for slot in range(2):
        for k in range(NSUB):
            ycopy(slot, k).wait_send()
        for q in range(1, 4):
            qcopy(slot, q, NCH - 2 + slot, me).wait_send()

    keep = pltpu.make_async_copy(t3, t_out, osem)
    keep.start()

    acc = lax.dot_general(y1b[0], y1b[0], NT, preferred_element_type=F32)
    for c in range(1, CL // 2):
        acc = acc + lax.dot_general(y1b[c], y1b[c], NT, preferred_element_type=F32)
    gram[...] = acc

    def rows_of(dev):
        return pl.ds(pl.multiple_of(flat(dev) * RT, 8), RT)

    def gcopy(k):
        return remote(gram.at[rows_of(peer(me, k))], gslots.at[k - 1], gsend.at[k - 1], grecv.at[k - 1], peer(me, k))

    for k in range(1, 8):
        gcopy(k).start()
    total = gram[rows_of(me), :]
    for k in range(1, 8):
        gcopy(k).wait_recv()
        total = total + gslots[k - 1]
    pall[flat(me)] = jnp.dot(total.astype(BF16), u1_ref[...], preferred_element_type=F32)

    def pcopy(k, dev):
        return remote(pall.at[flat(me)], pall.at[flat(dev)], psend.at[k - 1], precv.at[k - 1], peer(me, k))

    for k in range(1, 8):
        pcopy(k, me).start()
    for k in range(1, 8):
        pcopy(k, peer(me, k)).wait_recv()
    power = pall[...].reshape(8 * RT, 128)[:, :RT]
    u1_out[...] = power / jnp.sqrt(jnp.sum(power * power, axis=0, keepdims=True))
    for k in range(1, 8):
        gcopy(k).wait_send()
        pcopy(k, me).wait_send()
    keep.wait()


def time_phase(x2d, u3t, u2p, u1p):
    vmem, anym = pl.BlockSpec(memory_space=pltpu.VMEM), pl.BlockSpec(memory_space=pl.ANY)
    dma = pltpu.SemaphoreType.DMA
    return pl.pallas_call(
        time_kernel,
        name='time_phase',
        out_shape=(jax.ShapeDtypeStruct((2, NCH, 2, CL * CH, HP), BF16), jax.ShapeDtypeStruct((2 * FR, RT), F32)),
        in_specs=[anym, vmem, vmem, vmem],
        out_specs=(anym, vmem),
        scratch_shapes=[
            pltpu.VMEM((NSUB, SUB, GW), BF16), pltpu.VMEM((2, CW, POS), F32), pltpu.VMEM((2, CW, POS), F32), pltpu.VMEM((2, CW, POS), F32),
            pltpu.VMEM((3, CW * CH, 128), F32), pltpu.VMEM((2, 3, CL * CH, HP), BF16), pltpu.VMEM((2, NCH, 2, CL * CH, HP), BF16),
            pltpu.VMEM((CL // 2, 2 * FR, 256), BF16), pltpu.VMEM((2 * FR, 2 * FR), F32), pltpu.VMEM((7, RT, 2 * FR), F32), pltpu.VMEM((8, RT, 128), F32),
            dma((NSUB,)), dma((2, NSUB)), dma((2, NSUB)), pltpu.SemaphoreType.REGULAR, dma((2, 3)), dma((3, NCH)),
            dma((7,)), dma((7,)), dma((7,)), dma((7,)), dma(()),
        ],
        compiler_params=pltpu.CompilerParams(collective_id=0, has_side_effects=True, vmem_limit_bytes=60 << 20),
    )(x2d, u3t, u2p, u1p)


HB = 8
NHB = GH // HB
GQ = 96
TN = (((0,), (0,)), ((), ()))
TG = 4
AT_CHIP, AT_POWER = 4, 22


def height_kernel(t_hbm, x_hbm, u1t_ref, u1z_ref, u2p_ref, u2_out, z_out, t3, y2, gram, core_in, chip_in, pall, kron, xbuf, zown, zsend, zrecv, zb,
                  tsem, csend, crecv, gsend, grecv, psend, precv, xsem, dsend, drecv, credit, osem):
    me = coords()
    y, x, a = me
    c_peer = peer(me, 1)
    chips = (2, 4, 6)
    greet_all(me)
    width = CL * CH // TG

    def tcopy(g):
        rows = pl.ds(g * width, width)
        return pltpu.make_async_copy(t_hbm.at[:, :, :, rows, :], t3.at[:, :, :, rows, :], tsem.at[g])

    def fetch(b):
        slot = lax.rem(b, 3)
        return pltpu.make_async_copy(x_hbm.at[:, pl.ds(pl.multiple_of(b * HB, HB), HB), :], xbuf.at[slot], xsem.at[slot])

    for g in range(TG):
        tcopy(g).start()
    fetch(0).start()
    fetch(1).start()

    def one_hot(shape, dim, step):
        return (lax.broadcasted_iota(jnp.int32, shape, dim) // step == lax.broadcasted_iota(jnp.int32, shape, 1 - dim)).astype(BF16)

    rep = jnp.dot(one_hot((RT * HB, RT), 0, HB), u1z_ref[...], preferred_element_type=F32).astype(BF16)
    for i in range(0, FR * HB, 512):
        cols = lax.broadcasted_iota(jnp.int32, (FR, 512), 1) + i
        spread = (cols // HB == lax.broadcasted_iota(jnp.int32, (FR, 512), 0)).astype(BF16)
        wide = jnp.dot(rep, spread, preferred_element_type=F32)
        row = lax.broadcasted_iota(jnp.int32, (RT * HB, 512), 0)
        col = lax.broadcasted_iota(jnp.int32, (RT * HB, 512), 1)
        kron[:, i:i + 512] = jnp.where(lax.rem(row, HB) == lax.rem(col, HB), wide, 0.0).astype(BF16)

    for g in range(TG):
        tcopy(g).wait()

        def column(c, carry):
            for xh in range(2):
                frames = t3[:, :, xh, pl.ds(pl.multiple_of(c * CH, CH), CH), :].reshape(2 * FR, HP)
                y2[c, :, xh * HP:(xh + 1) * HP] = jnp.dot(u1t_ref[...], frames, preferred_element_type=F32).astype(BF16)
            return carry

        lax.fori_loop(g * (CL // TG), (g + 1) * (CL // TG), column, 0)

    def gram_block(m, carry):
        cols = pl.ds(pl.multiple_of(m * 128, 128), 128)
        lhs = y2[:, :, cols].reshape(CL * RT, 128)
        gram[cols, :] = lax.dot_general(lhs, y2[...].reshape(CL * RT, 2 * HP), TN, preferred_element_type=F32)
        return carry

    lax.fori_loop(0, 2 * HP // 128, gram_block, 0)

    def half_of(core):
        return pl.ds(pl.multiple_of(core * HP, HP), HP)

    def rows_of(dev):
        return pl.ds(pl.multiple_of(a * HP + (dev[1] * 2 + dev[0]) * GQ, 8), GQ)

    def slot_of(dev):
        return dev[2] * 4 + dev[1] * 2 + dev[0]

    ccopy = remote(gram.at[half_of(1 - a)], core_in, csend, crecv, c_peer)

    def gcopy(i):
        dev = peer(me, chips[i])
        return remote(gram.at[rows_of(dev)], chip_in.at[i], gsend.at[i], grecv.at[i], dev)

    def pcopy(k, dev):
        return remote(pall.at[slot_of(dev)], pall.at[slot_of(dev)], psend.at[k - 1], precv.at[k - 1], peer(me, k))

    ccopy.start()

    def zcopy(slot):
        return remote(zsend.at[slot], zrecv.at[slot], dsend.at[slot], drecv.at[slot], c_peer)

    def zput(b):
        slot = lax.rem(b, 2)
        return pltpu.make_async_copy(zb.at[slot], z_out.at[:, pl.ds(pl.multiple_of(b * HB, HB), HB), :], osem.at[slot])

    def zblock(b, carry):
        @pl.when(b < NHB)
        def _():
            slot = lax.rem(b, 3)
            fetch(b).wait()

            @pl.when(b < NHB - 2)
            def _():
                fetch(b + 2).start()

            @pl.when(b >= 3)
            def _():
                pl.semaphore_wait(credit, 1)
                zcopy(slot).wait_send()

            part = jnp.dot(kron[...], xbuf[slot].reshape(FR * HB, GW), preferred_element_type=F32)
            zown[slot] = part[:FR]
            zsend[slot] = part[FR:]
            zcopy(slot).start()

        @pl.when(b >= 1)
        def _():
            slot = lax.rem(b - 1, 3)
            zcopy(slot).wait_recv()

            @pl.when(b >= 3)
            def _():
                zput(b - 3).wait()

            zb[lax.rem(b - 1, 2)] = (zown[slot] + zrecv[slot]).astype(BF16).reshape(RT // 2, HB, GW)
            zput(b - 1).start()

            @pl.when(b - 1 < NHB - 3)
            def _():
                pl.semaphore_signal(credit, inc=1, device_id=c_peer, device_id_type=MESH)

        @pl.when(b == AT_CHIP)
        def _():
            ccopy.wait_recv()
            gram[half_of(a), :] += core_in[...]
            for i in range(3):
                gcopy(i).start()

        @pl.when(b == AT_POWER)
        def _():
            total = gram[rows_of(me), :]
            for i in range(3):
                gcopy(i).wait_recv()
                total = total + chip_in[i]
            pall[slot_of(me)] = jnp.dot(total.astype(BF16), u2p_ref[...], preferred_element_type=F32)
            for k in range(1, 8):
                pcopy(k, me).start()

        return carry

    lax.fori_loop(0, NHB + 1, zblock, 0)

    for k in range(1, 8):
        pcopy(k, peer(me, k)).wait_recv()
    power = pall[...].reshape(2 * HP, 128)[:, :RH]
    fresh = power / jnp.sqrt(jnp.sum(power * power, axis=0, keepdims=True))
    u2_out[0:GH, :] = fresh[0:GH]
    u2_out[GH:2 * GH, :] = fresh[HP:HP + GH]

    ccopy.wait_send()
    for i in range(3):
        gcopy(i).wait_send()
        zcopy(i).wait_send()
    for k in range(1, 8):
        pcopy(k, me).wait_send()
    zput(NHB - 2).wait()
    zput(NHB - 1).wait()


def height_phase(t3, tensor, u1t, u1z, u2p):
    vmem, anym = pl.BlockSpec(memory_space=pltpu.VMEM), pl.BlockSpec(memory_space=pl.ANY)
    dma = pltpu.SemaphoreType.DMA
    return pl.pallas_call(
        height_kernel,
        name='height_phase',
        out_shape=(jax.ShapeDtypeStruct((2 * GH, RH), F32), jax.ShapeDtypeStruct((RT // 2, GH, GW), BF16)),
        in_specs=[anym, anym, vmem, vmem, vmem],
        out_specs=(vmem, anym),
        scratch_shapes=[
            pltpu.VMEM((2, NCH, 2, CL * CH, HP), BF16), pltpu.VMEM((CL, RT, 2 * HP), BF16), pltpu.VMEM((2 * HP, 2 * HP), F32), pltpu.VMEM((HP, 2 * HP), F32),
            pltpu.VMEM((3, GQ, 2 * HP), F32), pltpu.VMEM((8, GQ, 128), F32), pltpu.VMEM((RT * HB, FR * HB), BF16), pltpu.VMEM((3, FR, HB, GW), BF16),
            pltpu.VMEM((3, FR, GW), F32), pltpu.VMEM((3, FR, GW), F32), pltpu.VMEM((3, FR, GW), F32), pltpu.VMEM((2, RT // 2, HB, GW), BF16),
            dma((TG,)), dma(()), dma(()), dma((3,)), dma((3,)), dma((7,)), dma((7,)), dma((3,)), dma((3,)), dma((3,)), pltpu.SemaphoreType.REGULAR, dma((2,)),
        ],
        compiler_params=pltpu.CompilerParams(collective_id=2, has_side_effects=True, vmem_limit_bytes=60 << 20),
    )(t3, tensor, u1t, u1z, u2p)


NPAIR = 12
PR = RH
WP = 768
WQ = WP // 4


def width_kernel(z_hbm, u2t_ref, u3p_ref, u3_out, g_out, e_out, zbuf, own, send, recv, y3, acc, core_in, x_in, pall, u3b, energy,
                 zsem, xsend, xrecv, ysend, yrecv, csend, crecv, rsend, rrecv, psend, precv, fsend, frecv, esend, erecv):
    me = coords()
    y, x, a = me
    x_peer, y_peer, c_peer = peer(me, 2), peer(me, 4), peer(me, 1)
    greet_all(me)

    def fetch(p, slot):
        return pltpu.make_async_copy(z_hbm.at[pl.ds(p * 2, 2)], zbuf.at[slot], zsem.at[slot])

    def xcopy(p):
        return remote(send.at[p], recv.at[p], xsend.at[p], xrecv.at[p], x_peer)

    def ycopy(p):
        return remote(y3.at[0, p], y3.at[1, p], ysend.at[p], yrecv.at[p], y_peer)

    fetch(0, 0).start()
    acc[...] = jnp.zeros_like(acc)

    def produce(p, carry):
        slot = lax.rem(p, 2)
        fetch(p, slot).wait()

        @pl.when(p < NPAIR - 1)
        def _():
            fetch(p + 1, 1 - slot).start()

        for r in range(2):
            part = jnp.dot(u2t_ref[...], zbuf[slot, r], preferred_element_type=F32)
            own[p, r * 44:(r + 1) * 44] = part[0:44]
            send[p, r * 44:(r + 1) * 44] = part[48:92]
        xcopy(p).start()
        return carry

    lax.fori_loop(0, NPAIR, produce, 0)

    def add_gram(p):
        ycopy(p).wait_recv()

        def block(m, carry):
            cols = pl.ds(pl.multiple_of(m * 128, 128), 128)
            lhs = y3[0, p, :, cols]
            for half in range(2):
                add = lax.dot_general(lhs, y3[half, p], (((0,), (0,)), ((), ())), preferred_element_type=F32)
                acc[cols, half * WP:(half + 1) * WP] += add
            return carry

        lax.fori_loop(0, WP // 128, block, 0)

    def consume(p, carry):
        @pl.when(p < NPAIR)
        def _():
            xcopy(p).wait_recv()
            y3[0, p, :, 640:768] = jnp.zeros((PR, 128), BF16)
            y3[0, p, :, 0:GW] = (own[p] + recv[p]).astype(BF16)
            ycopy(p).start()

        @pl.when(p >= 1)
        def _():
            add_gram(p - 1)

        return carry

    lax.fori_loop(0, NPAIR + 1, consume, 0)

    def quarter(core, side):
        return pl.ds(pl.multiple_of(core * 2 * WQ + side * WQ, 8), WQ)

    def ccopy(i):
        side = 1 - x if i == 0 else x
        return remote(acc.at[quarter(1 - a, side)], core_in.at[i], csend.at[i], crecv.at[i], c_peer)

    ccopy(0).start()
    ccopy(1).start()
    ccopy(0).wait_recv()
    acc[quarter(a, 1 - x), :] += core_in[0]
    rcopy = remote(acc.at[quarter(a, 1 - x)], x_in, rsend, rrecv, x_peer)
    rcopy.start()
    ccopy(1).wait_recv()
    rows = acc[quarter(a, x), :] + core_in[1]
    rcopy.wait_recv()
    rows = (rows + x_in[...]).astype(BF16)

    def slot_of(dev):
        return dev[0] * 4 + dev[2] * 2 + dev[1]

    mine = slot_of(me)
    pall[mine] = jnp.dot(rows, u3p_ref[...], preferred_element_type=F32)

    def pcopy(i, dev):
        return remote(pall.at[slot_of(dev)], pall.at[slot_of(dev)], psend.at[i], precv.at[i], peer(me, (2, 4, 6)[i]))

    def fcopy(i, dev):
        return remote(pall.at[slot_of(dev)], pall.at[slot_of(dev)], fsend.at[i], frecv.at[i], c_peer)

    for i in range(3):
        pcopy(i, me).start()
    fcopy(3, me).start()
    for i in range(3):
        dev = peer(me, (2, 4, 6)[i])
        pcopy(i, dev).wait_recv()
        fcopy(i, dev).start()
    for i in range(3):
        fcopy(i, peer(c_peer, (2, 4, 6)[i])).wait_recv()
    fcopy(3, c_peer).wait_recv()
    power = pall[...].reshape(2 * WP, 256)
    lane = lax.broadcasted_iota(jnp.int32, (1, 256), 1)
    norm = jnp.where(lane < RW, jnp.sqrt(jnp.sum(power * power, axis=0, keepdims=True)), 1.0)
    fresh = power / norm
    u3_out[0:GW, :] = fresh[0:GW, :RW]
    u3_out[GW:2 * GW, :] = fresh[WP:WP + GW, :RW]
    half = pltpu.roll(fresh, 256 - y * CW, 1)[:, :128].astype(BF16)
    u3b[...] = half.reshape(2, WP, 128)

    def core_rows(p, esum):
        g = jnp.dot(y3[0, p], u3b[y], preferred_element_type=F32) + jnp.dot(y3[1, p], u3b[1 - y], preferred_element_type=F32)
        g = jnp.where(lane[:, :128] < CW, g, 0.0)
        g_out[p] = g[:, :CW]
        return esum + jnp.sum((g * g).reshape(PR // 8, 8, 128), axis=0)

    energy[flat(me)] = lax.fori_loop(0, NPAIR, core_rows, jnp.zeros((8, 128), F32))

    def ecopy(k, dev):
        return remote(energy.at[flat(dev)], energy.at[flat(dev)], esend.at[k - 1], erecv.at[k - 1], peer(me, k))

    for k in range(1, 8):
        ecopy(k, me).start()
    for k in range(1, 8):
        ecopy(k, peer(me, k)).wait_recv()
    e_out[...] = jnp.sum(jnp.sum(energy[...], axis=0), axis=(0, 1), keepdims=True)

    def drain(p, carry):
        xcopy(p).wait_send()
        ycopy(p).wait_send()
        return carry

    lax.fori_loop(0, NPAIR, drain, 0)
    ccopy(0).wait_send()
    ccopy(1).wait_send()
    rcopy.wait_send()
    for i in range(3):
        pcopy(i, me).wait_send()
    for i in range(4):
        fcopy(i, me).wait_send()
    for k in range(1, 8):
        ecopy(k, me).wait_send()


def width_phase(z_mat, u2t, u3p):
    vmem, anym = pl.BlockSpec(memory_space=pltpu.VMEM), pl.BlockSpec(memory_space=pl.ANY)
    dma = pltpu.SemaphoreType.DMA
    return pl.pallas_call(
        width_kernel,
        name='width_phase',
        out_shape=(jax.ShapeDtypeStruct((2 * GW, RW), F32), jax.ShapeDtypeStruct((NPAIR, PR, CW), F32), jax.ShapeDtypeStruct((1, 1), F32)),
        in_specs=[anym, vmem, vmem],
        out_specs=(vmem, vmem, vmem),
        scratch_shapes=[
            pltpu.VMEM((2, 2, GH, GW), BF16), pltpu.VMEM((NPAIR, PR, GW), F32), pltpu.VMEM((NPAIR, PR, GW), F32), pltpu.VMEM((NPAIR, PR, GW), F32),
            pltpu.VMEM((2, NPAIR, PR, WP), BF16), pltpu.VMEM((WP, 2 * WP), F32), pltpu.VMEM((2, WQ, 2 * WP), F32), pltpu.VMEM((WQ, 2 * WP), F32),
            pltpu.VMEM((8, WQ, 256), F32), pltpu.VMEM((2, WP, 128), BF16), pltpu.VMEM((8, 8, 128), F32),
            dma((2,)), dma((NPAIR,)), dma((NPAIR,)), dma((NPAIR,)), dma((NPAIR,)), dma((2,)), dma((2,)), dma(()), dma(()),
            dma((3,)), dma((3,)), dma((4,)), dma((4,)), dma((7,)), dma((7,)),
        ],
        compiler_params=pltpu.CompilerParams(collective_id=1, has_side_effects=True, vmem_limit_bytes=60 << 20),
    )(z_mat, u2t, u3p)


def rows_of(factor, axis_name, count):
    start_row = lax.axis_index(axis_name) * count
    return lax.dynamic_slice_in_dim(factor, start_row, count, 0).astype(BF16)


def solution(mesh):
    def local_sweep(tensor, u_time, u_height, u_width):
        frames, grid_h, grid_w = tensor.shape
        y = lax.axis_index('a3')
        u3 = rows_of(u_width, 'a3', grid_w).T
        u3t = jnp.concatenate([lax.dynamic_slice_in_dim(u3, y * CW, CW, 0), lax.dynamic_slice_in_dim(u3, (1 - y) * CW, CW, 0)], 0)
        u2p = jnp.pad(u_height.astype(BF16).reshape(2, grid_h, RH), ((0, 0), (0, HP - grid_h), (0, 128 - RH)))
        u1p = jnp.pad(u_time.astype(BF16), ((0, 0), (0, 128 - RT)))
        t3, new_time = time_phase(tensor.reshape(frames * grid_h, grid_w), u3t, u2p, u1p)
        u1t = new_time.astype(BF16).T
        a = lax.axis_index('a1')
        local = lax.dynamic_slice_in_dim(u1t, a * frames, frames, 1)
        half = RT // 2
        u1z = jnp.concatenate([lax.dynamic_slice_in_dim(local, a * half, half, 0), lax.dynamic_slice_in_dim(local, (1 - a) * half, half, 0)], 0)
        new_height, z_mat = height_phase(t3, tensor, u1t, u1z, u2p.reshape(2 * HP, 128))
        x = lax.axis_index('a2')
        u2r = rows_of(new_height, 'a2', grid_h).T
        own_b, other_b = lax.dynamic_slice_in_dim(u2r, x * 44, 44, 0), lax.dynamic_slice_in_dim(u2r, (1 - x) * 44, 44, 0)
        u2t = jnp.concatenate([jnp.pad(own_b, ((0, 4), (0, 0))), jnp.pad(other_b, ((0, 4), (0, 0)))], 0)
        u3y = jnp.pad(u_width.astype(BF16).reshape(2, grid_w, RW), ((0, 0), (0, WP - grid_w), (0, 256 - RW)))
        u3p = jnp.concatenate([lax.dynamic_slice_in_dim(u3y, y, 1, 0), lax.dynamic_slice_in_dim(u3y, 1 - y, 1, 0)], 0).reshape(2 * WP, 256)
        new_width, core_tensor, core_energy = width_phase(z_mat, u2t, u3p)
        core_tensor = core_tensor.reshape(RT // 2, RH // 2, CW)
        core_energy = core_energy.reshape(())
        return new_time, new_height, new_width, core_tensor, core_energy

    return jax.shard_map(local_sweep, mesh=mesh, in_specs=(P('a1', 'a2', 'a3'), P(), P(), P()), out_specs=(P(), P(), P(), P('a1', 'a2', 'a3'), P()), check_vma=False)
```
